8 devices in a mesh: rep: 1 (over z), fsdp: 8 (over y, x, core).
Axes of the slice: x: 2, y: 2, z: 1, core: 2. Of those that a mesh axis runs over, the one named last changes fastest.
Arguments:
- act_in: bfloat16 [12, 4096, 3072], P(None, ('rep', 'fsdp'))
- cot_out: bfloat16 [12, 4096, 3072], P(None, ('rep', 'fsdp'))
- lengths: int32 [12, 8], P(None, ('rep', 'fsdp'))
- w_in: bfloat16 [1, 3072, 8192], P(None, 'fsdp')
- w_out: bfloat16 [1, 8192, 3072], P(None, 'fsdp')
Outputs:
- output 1: float32 [1, 3072, 8192], P(None, ('rep', 'fsdp'))
- output 2: float32 [1, 8192, 3072], P(None, ('rep', 'fsdp'))
All inputs are finite; a program needn't handle non-finite values.
Results may differ from the reference program's by a relative error of at most 0.00939663.
Values are sent between devices in bfloat16 or wider.
A program may use at most 1 GiB of HBM per device.

```python
import math
import jax
import jax.numpy as jnp
from jax import lax

MICRO_BATCHES = 12
TOKENS_DEV = 512
GROUP_DEVS = 8
D_MODEL = 3072
D_FF = 8192
LAYERS = 1

GROUP_TOKENS = TOKENS_DEV * GROUP_DEVS
MIN_LEN = TOKENS_DEV // 8
COT_SCALE = (MICRO_BATCHES * GROUP_TOKENS) ** -0.5
SQRT_HALF = math.sqrt(0.5)
INV_SQRT_TAU = 1.0 / math.sqrt(2.0 * math.pi)


def gelu_fwd(pre_act):
    return 0.5 * pre_act * (1.0 + lax.erf(pre_act * SQRT_HALF))


def gelu_grad(pre_act):
    return 0.5 * (1.0 + lax.erf(pre_act * SQRT_HALF)) + pre_act * jnp.exp(-0.5 * pre_act * pre_act) * INV_SQRT_TAU


def draw_lengths(key):
    k_draw, k_long, k_short = jax.random.split(key, 3)
    slot_count = MICRO_BATCHES * GROUP_DEVS
    len_draw = jax.random.randint(k_draw, (slot_count,), MIN_LEN, TOKENS_DEV + 1)
    long_pos = jax.random.randint(k_long, (), 0, slot_count)
    short_pos = (long_pos + jax.random.randint(k_short, (), 1, slot_count)) % slot_count
    slot_idx = jnp.arange(slot_count)
    len_draw = jnp.where(slot_idx == long_pos, TOKENS_DEV, len_draw)
    len_draw = jnp.where(slot_idx == short_pos, MIN_LEN, len_draw)
    return len_draw.reshape(MICRO_BATCHES, GROUP_DEVS).astype(jnp.int32)


def setup_inputs(seed: int = 0, part: int = 0) -> dict:
    base_key = jax.random.key(seed)
    part_key = jax.random.fold_in(base_key, part)
    k_act, k_cot, k_len = jax.random.split(part_key, 3)
    k_up, k_down = jax.random.split(jax.random.key(seed + 1), 2)
    act_in = jax.random.normal(k_act, (MICRO_BATCHES, GROUP_TOKENS, D_MODEL), jnp.float32)
    cot_out = jax.random.normal(k_cot, (MICRO_BATCHES, GROUP_TOKENS, D_MODEL), jnp.float32) * COT_SCALE
    w_in = jax.random.normal(k_up, (LAYERS, D_MODEL, D_FF), jnp.float32) * D_MODEL ** -0.5
    w_out = jax.random.normal(k_down, (LAYERS, D_FF, D_MODEL), jnp.float32) * D_FF ** -0.5
    return {
        'act_in': act_in.astype(jnp.bfloat16),
        'cot_out': cot_out.astype(jnp.bfloat16),
        'lengths': draw_lengths(k_len),
        'w_in': w_in.astype(jnp.bfloat16),
        'w_out': w_out.astype(jnp.bfloat16),
    }


def reference(act_in, cot_out, lengths, w_in, w_out):
    block_count = MICRO_BATCHES * GROUP_DEVS
    act_blocks = act_in.reshape(block_count, TOKENS_DEV, D_MODEL)
    cot_blocks = cot_out.reshape(block_count, TOKENS_DEV, D_MODEL)
    len_blocks = lengths.reshape(block_count)
    tok_pos = jnp.arange(TOKENS_DEV)

    def fwd_layer(hidden, weights):
        w_up, w_down = weights
        pre_act = jnp.dot(hidden, w_up, preferred_element_type=jnp.float32).astype(jnp.bfloat16)
        post_act = gelu_fwd(pre_act.astype(jnp.float32)).astype(jnp.bfloat16)
        hidden_next = (hidden.astype(jnp.float32) + jnp.dot(post_act, w_down, preferred_element_type=jnp.float32)).astype(jnp.bfloat16)
        return hidden_next, (hidden, pre_act, post_act)

    def bwd_layer(cot_cur, items):
        w_up, w_down, hidden, pre_act, post_act = items
        grad_down = jnp.dot(post_act.T, cot_cur, preferred_element_type=jnp.float32)
        d_act = jnp.dot(cot_cur, w_down.T, preferred_element_type=jnp.float32)
        d_pre = (d_act * gelu_grad(pre_act.astype(jnp.float32))).astype(jnp.bfloat16)
        grad_up = jnp.dot(hidden.T, d_pre, preferred_element_type=jnp.float32)
        cot_prev = (cot_cur.astype(jnp.float32) + jnp.dot(d_pre, w_up.T, preferred_element_type=jnp.float32)).astype(jnp.bfloat16)
        return cot_prev, (grad_up, grad_down)

    def one_block(carry, block_in):
        acc_in, acc_out = carry
        act_blk, cot_blk, len_blk = block_in
        cot_kept = jnp.where((tok_pos < len_blk)[:, None], cot_blk, jnp.zeros_like(cot_blk))
        hidden_last, saved = lax.scan(fwd_layer, act_blk, (w_in, w_out))
        cot_first, grads = lax.scan(bwd_layer, cot_kept, (w_in, w_out) + saved, reverse=True)
        return (acc_in + grads[0], acc_out + grads[1]), None

    init_acc = (jnp.zeros((LAYERS, D_MODEL, D_FF), jnp.float32), jnp.zeros((LAYERS, D_FF, D_MODEL), jnp.float32))
    totals, unused_out = lax.scan(one_block, init_acc, (act_blocks, cot_blocks, len_blocks))
    return totals[0], totals[1]
```

```python
import functools
import math
import jax
import jax.numpy as jnp
from jax import lax
from jax.experimental import pallas as pl
from jax.experimental.pallas import tpu as pltpu
from jax.sharding import PartitionSpec as P

SQRT_HALF = math.sqrt(0.5)
INV_SQRT_TAU = 1.0 / math.sqrt(2.0 * math.pi)

CHUNKS = 4
BLOCK = 512
ALIGN = 16
VMEM_LIMIT = 66 * 1024 * 1024 - 2 * 1024 * 1024 - 65536


def pack_kernel(meta, x_ref, e_ref, *refs, micro, tok, last_call):
    x_out, e_out, x_buf, e_buf, sems = refs[-5:]
    k = pl.program_id(0)
    bits = [1 << b for b in range(tok.bit_length() - 1, ALIGN.bit_length() - 2, -1)]

    def segment(step, act):
        slot = lax.rem(step, 2)
        rows = jnp.bitwise_and(meta[step] + (ALIGN - 1), -ALIGN)
        offset = meta[micro + step]
        for bit in bits:
            @pl.when(jnp.bitwise_and(rows, bit) != 0)
            def _():
                first = pl.multiple_of(jnp.bitwise_and(rows, -2 * bit), ALIGN)
                dest = pl.multiple_of(offset + first, ALIGN)
                for n, (buf, out) in enumerate(((x_buf, x_out), (e_buf, e_out))):
                    act(pltpu.make_async_copy(buf.at[slot, pl.ds(first, bit)], out.at[pl.ds(dest, bit)], sems.at[n, slot]))

    @pl.when(k >= 2)
    def _():
        segment(k - 2, lambda copy: copy.wait())

    slot = lax.rem(k, 2)
    x_buf[slot] = x_ref[0]
    e_buf[slot] = e_ref[0]
    length = meta[k]
    edge = pl.multiple_of(jnp.minimum(jnp.bitwise_and(length, -ALIGN), tok - ALIGN), ALIGN)
    row = edge + lax.broadcasted_iota(jnp.int32, (ALIGN, x_buf.shape[-1]), 0)
    for buf in (x_buf, e_buf):
        kept = jnp.where(row < length, buf[slot, pl.ds(edge, ALIGN)].astype(jnp.float32), 0.0)
        buf[slot, pl.ds(edge, ALIGN)] = kept.astype(buf.dtype)
    segment(k, lambda copy: copy.start())

    @pl.when(k == micro - 1)
    def _():
        segment(k - 1, lambda copy: copy.wait())
        segment(k, lambda copy: copy.wait())
        if last_call:
            total, gap = meta[2 * micro], meta[2 * micro + 1]
            x_buf[0] = jnp.zeros(x_buf.shape[1:], x_buf.dtype)

            def tail(act):
                for bit in bits[1:]:
                    @pl.when(jnp.bitwise_and(gap, bit) != 0)
                    def _():
                        first = jnp.bitwise_and(gap, -2 * bit)
                        dest = pl.multiple_of(total + first, ALIGN)
                        for n, out in enumerate((x_out, e_out)):
                            act(pltpu.make_async_copy(x_buf.at[0, pl.ds(0, bit)], out.at[pl.ds(dest, bit)], sems.at[n, 0]))

            tail(lambda copy: copy.start())
            tail(lambda copy: copy.wait())


def pack(meta, x, e, packed, cap):
    micro, tok, width = x.shape
    hbm = pl.BlockSpec(memory_space=pltpu.MemorySpace.HBM)
    block = pl.BlockSpec((1, tok, width), lambda k, meta: (k, 0, 0))
    given = () if packed is None else packed
    return pl.pallas_call(
        functools.partial(pack_kernel, micro=micro, tok=tok, last_call=packed is not None),
        grid_spec=pltpu.PrefetchScalarGridSpec(
            num_scalar_prefetch=1,
            grid=(micro,),
            in_specs=[block, block] + [hbm] * len(given),
            out_specs=[hbm, hbm],
            scratch_shapes=[
                pltpu.VMEM((2, tok, width), x.dtype),
                pltpu.VMEM((2, tok, width), x.dtype),
                pltpu.SemaphoreType.DMA((2, 2)),
            ],
        ),
        out_shape=[jax.ShapeDtypeStruct((cap, width), x.dtype)] * 2,
        input_output_aliases={} if packed is None else {3: 0, 4: 1},
        compiler_params=pltpu.CompilerParams(dimension_semantics=("arbitrary",), vmem_limit_bytes=40 * 1024 * 1024),
        cost_estimate=pl.CostEstimate(flops=30_000_000_000, bytes_accessed=4 * x.size, transcendentals=0),
        name="pack_own" if packed is None else "pack_partner",
    )(meta, x, e, *given)


def grads_kernel(meta, x_ref, e_ref, w1_hbm, w2_hbm, grads_hbm, w1, w2, acc_i, acc_o, act_t, dpre_t, sems):
    i = pl.program_id(0)
    slabs, _, slab_width = w1_hbm.shape
    width = w2.shape[1]
    parts = acc_i.shape[0]
    part_width = width // parts
    block = x_ref.shape[0]

    @pl.when(i == 0)
    def _():
        core = meta[1]
        copies = [pltpu.make_async_copy(w2_hbm, w2, sems.at[slabs])]
        for s in range(slabs):
            owner = 2 * (s // 2) + (core if s % 2 == 0 else 1 - core)
            column = pl.multiple_of(owner * slab_width, 128)
            copies.append(pltpu.make_async_copy(w1_hbm.at[s], w1.at[:, pl.ds(column, slab_width)], sems.at[s]))
        for copy in copies:
            copy.start()
        acc_i[...] = jnp.zeros_like(acc_i)
        acc_o[...] = jnp.zeros_like(acc_o)
        for copy in copies:
            copy.wait()

    @pl.when(i < meta[0])
    def _():
        sub = 256
        transposed = (((1,), (1,)), ((), ()))

        def hidden(t, carry):
            rows = pl.ds(pl.multiple_of(t * sub, sub), sub)
            pre = lax.dot_general(w1[...], x_ref[rows, :], transposed, preferred_element_type=jnp.float32)
            d_act = lax.dot_general(w2[...], e_ref[rows, :], transposed, preferred_element_type=jnp.float32)
            z = pre.astype(jnp.bfloat16).astype(jnp.float32)
            cdf = 0.5 * (1.0 + lax.erf(z * SQRT_HALF))
            slope = cdf + z * jnp.exp(-0.5 * z * z) * INV_SQRT_TAU
            act_t[:, rows] = (z * cdf).astype(jnp.bfloat16)
            dpre_t[:, rows] = (d_act * slope).astype(jnp.bfloat16)
            return carry

        lax.fori_loop(0, block // sub, hidden, 0)

        def accumulate(p, carry):
            columns = pl.ds(pl.multiple_of(p * part_width, 128), part_width)
            acc_o[p] += jnp.dot(act_t[...], e_ref[:, columns], preferred_element_type=jnp.float32)
            acc_i[p] += jnp.dot(dpre_t[...], x_ref[:, columns], preferred_element_type=jnp.float32)
            return carry

        lax.fori_loop(0, parts, accumulate, 0)

    @pl.when(i == pl.num_programs(0) - 1)
    def _():
        piece = acc_o.shape[1] // parts
        copies = [pltpu.make_async_copy(acc_i.at[q], grads_hbm.at[q, 0], sems.at[q]) for q in range(parts)]
        for q in range(parts):
            for p in range(parts):
                copies.append(pltpu.make_async_copy(
                    acc_o.at[p, pl.ds(q * piece, piece)], grads_hbm.at[q, 1, pl.ds(p * piece, piece)], sems.at[parts + q]))
        for copy in copies:
            copy.start()
        for copy in copies:
            copy.wait()


def chunk_grads(meta, x_packed, e_packed, w1_slabs, w2):
    cap, width = x_packed.shape
    hidden = w2.shape[0]
    slabs = w1_slabs.shape[0]
    parts = slabs // 2
    hbm = pl.BlockSpec(memory_space=pltpu.MemorySpace.HBM)
    tokens = pl.BlockSpec((BLOCK, width), lambda i, meta: (jnp.minimum(i, meta[0] - 1), 0))
    return pl.pallas_call(
        grads_kernel,
        grid_spec=pltpu.PrefetchScalarGridSpec(
            num_scalar_prefetch=1,
            grid=(cap // BLOCK,),
            in_specs=[tokens, tokens, hbm, hbm],
            out_specs=hbm,
            scratch_shapes=[
                pltpu.VMEM((hidden, width), jnp.bfloat16),
                pltpu.VMEM((hidden, width), jnp.bfloat16),
                pltpu.VMEM((parts, hidden, width // parts), jnp.float32),
                pltpu.VMEM((parts, hidden, width // parts), jnp.float32),
                pltpu.VMEM((hidden, BLOCK), jnp.bfloat16),
                pltpu.VMEM((hidden, BLOCK), jnp.bfloat16),
                pltpu.SemaphoreType.DMA((slabs + 1,)),
            ],
        ),
        out_shape=jax.ShapeDtypeStruct((parts, 2, hidden, width // parts), jnp.float32),
        compiler_params=pltpu.CompilerParams(dimension_semantics=("arbitrary",), vmem_limit_bytes=VMEM_LIMIT),
        cost_estimate=pl.CostEstimate(flops=8 * 7168 * width * hidden, bytes_accessed=8 * 7168 * width, transcendentals=0),
        name="chunk_grads",
    )(meta, x_packed, e_packed, w1_slabs, w2)


def turn_kernel(core, w_ref, out_ref):
    chunks, piece, _ = out_ref.shape
    for j in range(chunks):
        out_ref[j] = w_ref[:, j * piece:(j + 1) * piece].T


def turned_columns(core, w, other, chips):
    rows, full = w.shape
    per_device = full // (2 * chips)
    piece = per_device // CHUNKS
    return pl.pallas_call(
        turn_kernel,
        grid_spec=pltpu.PrefetchScalarGridSpec(
            num_scalar_prefetch=1,
            grid=(chips,),
            in_specs=[pl.BlockSpec((rows, per_device), lambda q, core: (0, 2 * q + jnp.bitwise_xor(core[0], other)))],
            out_specs=pl.BlockSpec((CHUNKS, piece, rows), lambda q, core: (0, q, 0)),
        ),
        out_shape=jax.ShapeDtypeStruct((CHUNKS, chips * piece, rows), w.dtype),
        compiler_params=pltpu.CompilerParams(dimension_semantics=("arbitrary",)),
        cost_estimate=pl.CostEstimate(flops=3_000_000_000, bytes_accessed=2 * w.size, transcendentals=0),
        name="turn_other" if other else "turn_own",
    )(core, w)


def place_kernel(core, kept_ref, got_ref, rows_ref, *refs):
    gi_ref, go_ref = refs[-2:]
    mine = pl.program_id(1) == core[0]

    @pl.when(mine)
    def _():
        gi_ref[...] = kept_ref[0].T

    @pl.when(jnp.logical_not(mine))
    def _():
        gi_ref[...] = got_ref[...].T

    go_ref[...] = rows_ref[0]


def place(core, reduced, got, outs, j, chips):
    _, hidden, part_width = reduced.shape
    piece = hidden // chips
    rows = part_width // 2
    given = () if outs is None else outs
    anywhere = pl.BlockSpec(memory_space=pltpu.MemorySpace.HBM)
    return pl.pallas_call(
        place_kernel,
        grid_spec=pltpu.PrefetchScalarGridSpec(
            num_scalar_prefetch=1,
            grid=(chips, 2),
            in_specs=[
                pl.BlockSpec((1, piece, rows), lambda q, c, core: (0, q, core[0])),
                pl.BlockSpec((piece, rows), lambda q, c, core: (q, 0)),
                pl.BlockSpec((1, piece, part_width), lambda q, c, core: (1, q, 0)),
            ] + [anywhere] * len(given),
            out_specs=[
                pl.BlockSpec((rows, piece), lambda q, c, core: (0, (2 * q + c) * CHUNKS + j)),
                pl.BlockSpec((piece, part_width), lambda q, c, core: (j, q)),
            ],
        ),
        out_shape=[
            jax.ShapeDtypeStruct((rows, 2 * CHUNKS * hidden), jnp.float32),
            jax.ShapeDtypeStruct((CHUNKS * piece, chips * part_width), jnp.float32),
        ],
        input_output_aliases={} if outs is None else {4: 0, 5: 1},
        compiler_params=pltpu.CompilerParams(dimension_semantics=("arbitrary", "arbitrary")),
        cost_estimate=pl.CostEstimate(flops=2_000_000_000, bytes_accessed=12 * reduced.size, transcendentals=0),
        name=f"place_{j}",
    )(core, reduced, got, reduced, *given)


def solution(mesh):
    shard_spec = P(None, ('rep', 'fsdp'), None)
    len_spec = P(None, ('rep', 'fsdp'))
    weight_spec = P(None, 'fsdp', None)
    count = mesh.shape['fsdp']
    chips = count // 2
    same_core = [[2 * q + c for q in range(chips)] for c in range(2)]
    swap = [(d, d ^ 1) for d in range(count)]

    def local_step(act_in, cot_out, lengths, w_in, w_out):
        micro, tok, width = act_in.shape
        core = lax.rem(lax.axis_index('fsdp'), 2)
        rows_in, rows_out = w_in.shape[1], w_out.shape[1]
        piece = rows_out // CHUNKS
        hidden = chips * piece

        lens = lengths[:, 0]
        lens_other = lax.ppermute(lens, 'fsdp', swap)
        x_other = lax.ppermute(act_in, 'fsdp', swap)
        e_other = lax.ppermute(cot_out, 'fsdp', swap)

        core_ref = core.reshape(1).astype(jnp.int32)
        w_got = lax.ppermute(turned_columns(core_ref, w_in[0], 1, chips), 'fsdp', swap)
        w_mine = turned_columns(core_ref, w_in[0], 0, chips)

        w2_parts, w1_parts = [], []
        for j in range(CHUNKS):
            w2_parts.append(lax.all_gather(w_out[0, j * piece:(j + 1) * piece], 'fsdp', axis=0, tiled=True, axis_index_groups=same_core))
            pair = jnp.stack([w_mine[j], w_got[j]])
            w1_parts.append(lax.all_gather(pair, 'fsdp', axis=0, tiled=True, axis_index_groups=same_core))

        def rounded(n):
            return (n + (ALIGN - 1)) // ALIGN * ALIGN

        cap = 2 * micro * tok
        all_rows = jnp.concatenate([rounded(lens), rounded(lens_other)])
        ends = jnp.cumsum(all_rows)
        starts = ends - all_rows
        total = ends[-1]
        blocks = (total + BLOCK - 1) // BLOCK
        edge = jnp.stack([total, blocks * BLOCK - total])
        packed = pack(jnp.concatenate([lens, starts[:micro], edge]), act_in, cot_out, None, cap)
        packed = pack(jnp.concatenate([lens_other, starts[micro:], edge]), x_other, e_other, packed, cap)
        meta = jnp.stack([blocks, core]).astype(jnp.int32)

        outs = None
        for j in range(CHUNKS):
            part = chunk_grads(meta, packed[0], packed[1], w1_parts[j], w2_parts[j])
            part = part.reshape(-1, part.shape[-1])
            reduced = lax.psum_scatter(part, 'fsdp', scatter_dimension=0, tiled=True, axis_index_groups=same_core)
            reduced = reduced.reshape(2, hidden, -1)
            away = lax.dynamic_slice_in_dim(reduced[0], (1 - core) * rows_in, rows_in, axis=1)
            got = lax.ppermute(away, 'fsdp', swap)
            outs = place(core_ref, reduced, got, outs, j, chips)
        return outs[0][None], outs[1][None]

    return jax.shard_map(local_step, mesh=mesh, in_specs=(shard_spec, shard_spec, len_spec, weight_spec, weight_spec), out_specs=(shard_spec, shard_spec), check_vma=False)
```

```python
import functools
import math
import jax
import jax.numpy as jnp
from jax import lax
from jax.experimental import pallas as pl
from jax.experimental.pallas import tpu as pltpu
from jax.sharding import PartitionSpec as P


SQRT_HALF = math.sqrt(0.5)
INV_SQRT_TAU = 1.0 / math.sqrt(2.0 * math.pi)

CHUNKS = 4
GATHERS = ((0, 1), (1, 2), (2, 4))
BLOCK = 512
ALIGN = 16
VMEM_LIMIT = 66 * 1024 * 1024 - 2 * 1024 * 1024 - 65536


def pack_kernel(meta, in_ref, *refs, micro, tok, last_call):
    out, buf, sems = refs[-3:]
    k = pl.program_id(0)
    bits = [1 << b for b in range(tok.bit_length() - 1, ALIGN.bit_length() - 2, -1)]

    def segment(step, act):
        slot = lax.rem(step, 2)
        rows = jnp.bitwise_and(meta[step] + (ALIGN - 1), -ALIGN)
        offset = meta[micro + step]
        for bit in bits:
            @pl.when(jnp.bitwise_and(rows, bit) != 0)
            def _():
                first = pl.multiple_of(jnp.bitwise_and(rows, -2 * bit), ALIGN)
                dest = pl.multiple_of(offset + first, ALIGN)
                act(pltpu.make_async_copy(buf.at[slot, pl.ds(first, bit)], out.at[pl.ds(dest, bit)], sems.at[slot]))

    @pl.when(k >= 2)
    def _():
        segment(k - 2, lambda copy: copy.wait())

    slot = lax.rem(k, 2)
    buf[slot] = in_ref[0]
    length = meta[k]
    edge = pl.multiple_of(jnp.minimum(jnp.bitwise_and(length, -ALIGN), tok - ALIGN), ALIGN)
    row = edge + lax.broadcasted_iota(jnp.int32, (ALIGN, buf.shape[-1]), 0)
    kept = jnp.where(row < length, buf[slot, pl.ds(edge, ALIGN)].astype(jnp.float32), 0.0)
    buf[slot, pl.ds(edge, ALIGN)] = kept.astype(buf.dtype)
    segment(k, lambda copy: copy.start())

    @pl.when(k == micro - 1)
    def _():
        segment(k - 1, lambda copy: copy.wait())
        segment(k, lambda copy: copy.wait())
        if last_call:
            total, gap = meta[2 * micro], meta[2 * micro + 1]
            buf[0] = jnp.zeros(buf.shape[1:], buf.dtype)

            def tail(act):
                for bit in bits[1:]:
                    @pl.when(jnp.bitwise_and(gap, bit) != 0)
                    def _():
                        first = jnp.bitwise_and(gap, -2 * bit)
                        dest = pl.multiple_of(total + first, ALIGN)
                        act(pltpu.make_async_copy(buf.at[0, pl.ds(0, bit)], out.at[pl.ds(dest, bit)], sems.at[0]))

            tail(lambda copy: copy.start())
            tail(lambda copy: copy.wait())


def pack(meta, tokens, packed, cap):
    micro, tok, width = tokens.shape
    hbm = pl.BlockSpec(memory_space=pltpu.MemorySpace.HBM)
    given = () if packed is None else (packed,)
    return pl.pallas_call(
        functools.partial(pack_kernel, micro=micro, tok=tok, last_call=packed is not None),
        grid_spec=pltpu.PrefetchScalarGridSpec(
            num_scalar_prefetch=1,
            grid=(micro,),
            in_specs=[pl.BlockSpec((1, tok, width), lambda k, meta: (k, 0, 0))] + [hbm] * len(given),
            out_specs=hbm,
            scratch_shapes=[pltpu.VMEM((2, tok, width), tokens.dtype), pltpu.SemaphoreType.DMA((2,))],
        ),
        out_shape=jax.ShapeDtypeStruct((cap, width), tokens.dtype),
        input_output_aliases={} if packed is None else {2: 0},
        compiler_params=pltpu.CompilerParams(dimension_semantics=("arbitrary",), vmem_limit_bytes=32 * 1024 * 1024),
        cost_estimate=pl.CostEstimate(flops=15_000_000_000, bytes_accessed=4 * tokens.size, transcendentals=0),
        name="pack_own" if packed is None else "pack_partner",
    )(meta, tokens, *given)


def grads_kernel(meta, x_ref, e_ref, w1_hbm, w2_hbm, grads_hbm, w1, w2, acc_i, acc_o, act_t, dpre_t, sems, *, w1_at, w2_at):
    i = pl.program_id(0)
    hidden_size, width = w2.shape
    slab_width = w1_hbm.shape[-1]
    parts = acc_i.shape[0]
    part_width = width // parts
    piece = hidden_size // parts
    block = x_ref.shape[0]

    @pl.when(i == 0)
    def _():
        core = meta[1]
        copies = []
        for q in range(parts):
            for k in range(2):
                column = pl.multiple_of((2 * q + (core if k == 0 else 1 - core)) * slab_width, 128)
                source = w1_hbm.at[q, w1_at[0], pl.ds(w1_at[1] + k * hidden_size, hidden_size)]
                copies.append(pltpu.make_async_copy(source, w1.at[:, pl.ds(column, slab_width)], sems.at[0]))
            if w2_at is None:
                continue
            for k in range(width // slab_width):
                source = w2_hbm.at[q, w2_at[0], pl.ds(w2_at[1] + k * piece, piece)]
                copies.append(pltpu.make_async_copy(source, w2.at[pl.ds(q * piece, piece), pl.ds(k * slab_width, slab_width)], sems.at[1]))
        if w2_at is None:
            copies.append(pltpu.make_async_copy(w2_hbm, w2, sems.at[1]))
        for copy in copies:
            copy.start()
        acc_i[...] = jnp.zeros_like(acc_i)
        acc_o[...] = jnp.zeros_like(acc_o)
        for copy in copies:
            copy.wait()

    @pl.when(i < meta[0])
    def _():
        sub = 256
        transposed = (((1,), (1,)), ((), ()))

        def hidden(t, carry):
            rows = pl.ds(pl.multiple_of(t * sub, sub), sub)
            pre = lax.dot_general(w1[...], x_ref[rows, :], transposed, preferred_element_type=jnp.float32)
            d_act = lax.dot_general(w2[...], e_ref[rows, :], transposed, preferred_element_type=jnp.float32)
            z = pre.astype(jnp.bfloat16).astype(jnp.float32)
            cdf = 0.5 * (1.0 + lax.erf(z * SQRT_HALF))
            slope = cdf + z * jnp.exp(-0.5 * z * z) * INV_SQRT_TAU
            act_t[:, rows] = (z * cdf).astype(jnp.bfloat16)
            dpre_t[:, rows] = (d_act * slope).astype(jnp.bfloat16)
            return carry

        lax.fori_loop(0, block // sub, hidden, 0)

        def results(p):
            yield pltpu.make_async_copy(acc_i.at[p], grads_hbm.at[p, 0], sems.at[0])
            for q in range(parts):
                yield pltpu.make_async_copy(
                    acc_o.at[p, pl.ds(q * piece, piece)],
                    grads_hbm.at[q, 1, pl.ds(pl.multiple_of(p * piece, 8), piece)], sems.at[1])

        last = i == meta[0] - 1

        def accumulate(p, carry):
            columns = pl.ds(pl.multiple_of(p * part_width, 128), part_width)
            acc_o[p] += jnp.dot(act_t[...], e_ref[:, columns], preferred_element_type=jnp.float32)
            acc_i[p] += jnp.dot(dpre_t[...], x_ref[:, columns], preferred_element_type=jnp.float32)

            @pl.when(last)
            def _():
                for copy in results(p):
                    copy.start()

            return carry

        lax.fori_loop(0, parts, accumulate, 0)

        @pl.when(last)
        def _():
            for p in range(parts):
                for copy in results(p):
                    copy.wait()


def chunk_grads(meta, x_packed, e_packed, w1_from, w1_at, w2_from, w2_at, hidden):
    cap, width = x_packed.shape
    parts = w1_from.shape[0]
    hbm = pl.BlockSpec(memory_space=pltpu.MemorySpace.HBM)
    tokens = pl.BlockSpec((BLOCK, width), lambda i, meta: (jnp.minimum(i, meta[0] - 1), 0))
    return pl.pallas_call(
        functools.partial(grads_kernel, w1_at=w1_at, w2_at=w2_at),
        grid_spec=pltpu.PrefetchScalarGridSpec(
            num_scalar_prefetch=1,
            grid=(cap // BLOCK,),
            in_specs=[tokens, tokens, hbm, hbm],
            out_specs=hbm,
            scratch_shapes=[
                pltpu.VMEM((hidden, width), jnp.bfloat16),
                pltpu.VMEM((hidden, width), jnp.bfloat16),
                pltpu.VMEM((parts, hidden, width // parts), jnp.float32),
                pltpu.VMEM((parts, hidden, width // parts), jnp.float32),
                pltpu.VMEM((hidden, BLOCK), jnp.bfloat16),
                pltpu.VMEM((hidden, BLOCK), jnp.bfloat16),
                pltpu.SemaphoreType.DMA((2,)),
            ],
        ),
        out_shape=jax.ShapeDtypeStruct((parts, 2, hidden, width // parts), jnp.float32),
        compiler_params=pltpu.CompilerParams(dimension_semantics=("arbitrary",), vmem_limit_bytes=VMEM_LIMIT),
        cost_estimate=pl.CostEstimate(flops=8 * 7168 * width * hidden, bytes_accessed=8 * 7168 * width, transcendentals=0),
        name="chunk_grads",
    )(meta, x_packed, e_packed, w1_from, w2_from)


def turn_kernel(core, w_ref, out_ref):
    chunks, piece, _ = out_ref.shape
    for j in range(chunks):
        out_ref[j] = w_ref[:, j * piece:(j + 1) * piece].T


def turned_columns(core, w, other, chips):
    rows, full = w.shape
    per_device = full // (2 * chips)
    piece = per_device // CHUNKS
    return pl.pallas_call(
        turn_kernel,
        grid_spec=pltpu.PrefetchScalarGridSpec(
            num_scalar_prefetch=1,
            grid=(chips,),
            in_specs=[pl.BlockSpec((rows, per_device), lambda q, core: (0, 2 * q + jnp.bitwise_xor(core[0], other)))],
            out_specs=pl.BlockSpec((CHUNKS, piece, rows), lambda q, core: (0, q, 0)),
        ),
        out_shape=jax.ShapeDtypeStruct((CHUNKS, chips * piece, rows), w.dtype),
        compiler_params=pltpu.CompilerParams(dimension_semantics=("arbitrary",)),
        cost_estimate=pl.CostEstimate(flops=3_000_000_000, bytes_accessed=2 * w.size, transcendentals=0),
        name="turn_other" if other else "turn_own",
    )(core, w)


def place_kernel(core, kept_ref, got_ref, rows_ref, *refs):
    gi_ref, go_ref = refs[-2:]
    mine = pl.program_id(1) == core[0]

    @pl.when(mine)
    def _():
        gi_ref[...] = kept_ref[0].T

    @pl.when(jnp.logical_not(mine))
    def _():
        gi_ref[...] = got_ref[...].T

    go_ref[...] = rows_ref[0]


def place(core, reduced, got, outs, j, chips):
    _, hidden, part_width = reduced.shape
    piece = hidden // chips
    rows = part_width // 2
    given = () if outs is None else outs
    anywhere = pl.BlockSpec(memory_space=pltpu.MemorySpace.HBM)
    return pl.pallas_call(
        place_kernel,
        grid_spec=pltpu.PrefetchScalarGridSpec(
            num_scalar_prefetch=1,
            grid=(chips, 2),
            in_specs=[
                pl.BlockSpec((1, piece, rows), lambda q, c, core: (0, q, core[0])),
                pl.BlockSpec((piece, rows), lambda q, c, core: (q, 0)),
                pl.BlockSpec((1, piece, part_width), lambda q, c, core: (1, q, 0)),
            ] + [anywhere] * len(given),
            out_specs=[
                pl.BlockSpec((rows, piece), lambda q, c, core: (0, (2 * q + c) * CHUNKS + j)),
                pl.BlockSpec((piece, part_width), lambda q, c, core: (j, q)),
            ],
        ),
        out_shape=[
            jax.ShapeDtypeStruct((rows, 2 * CHUNKS * hidden), jnp.float32),
            jax.ShapeDtypeStruct((CHUNKS * piece, chips * part_width), jnp.float32),
        ],
        input_output_aliases={} if outs is None else {4: 0, 5: 1},
        compiler_params=pltpu.CompilerParams(dimension_semantics=("arbitrary", "arbitrary")),
        cost_estimate=pl.CostEstimate(flops=2_000_000_000, bytes_accessed=12 * reduced.size, transcendentals=0),
    )(core, reduced, got, reduced, *given)


def solution(mesh):
    shard_spec = P(None, ('rep', 'fsdp'), None)
    len_spec = P(None, ('rep', 'fsdp'))
    weight_spec = P(None, 'fsdp', None)
    count = mesh.shape['fsdp']
    chips = count // 2
    same_core = [[2 * q + c for q in range(chips)] for c in range(2)]
    swap = [(d, d ^ 1) for d in range(count)]

    def local_step(act_in, cot_out, lengths, w_in, w_out):
        micro, tok, width = act_in.shape
        core = lax.rem(lax.axis_index('fsdp'), 2)
        rows_in, rows_out = w_in.shape[1], w_out.shape[1]
        piece = rows_out // CHUNKS
        hidden = chips * piece

        lens = lengths[:, 0]
        lens_other = lax.ppermute(lens, 'fsdp', swap)
        x_sent, e_sent, lens_other = lax.optimization_barrier((act_in, cot_out, lens_other))
        x_other = lax.ppermute(x_sent, 'fsdp', swap)
        e_other = lax.ppermute(e_sent, 'fsdp', swap)

        core_ref = core.reshape(1).astype(jnp.int32)
        w_got = lax.ppermute(turned_columns(core_ref, w_in[0], 1, chips), 'fsdp', swap)
        w_mine = turned_columns(core_ref, w_in[0], 0, chips)

        def gather(slabs):
            shape = slabs.shape
            flat = slabs.reshape(-1, shape[-1])
            flat = lax.all_gather(flat, 'fsdp', axis=0, tiled=True, axis_index_groups=same_core)
            return flat.reshape(chips, *shape)

        def out_rows(first, last):
            rows = w_out[0, first * piece:last * piece].reshape(last - first, piece, width // rows_in, rows_in)
            return rows.transpose(0, 2, 1, 3).reshape(last - first, -1, rows_in)

        weights = []
        for first, last in GATHERS:
            if first == 0:
                w2 = lax.all_gather(w_out[0, :piece], 'fsdp', axis=0, tiled=True, axis_index_groups=same_core)
                w1 = gather(jnp.concatenate([w_mine[:1], w_got[:1]], axis=1))
                weights.append((w1, (0, 0), w2, None))
            else:
                both = gather(jnp.concatenate([w_mine[first:last], w_got[first:last], out_rows(first, last)], axis=1))
                weights += [(both, (n, 0), both, (n, 2 * hidden)) for n in range(last - first)]

        def rounded(n):
            return (n + (ALIGN - 1)) // ALIGN * ALIGN

        cap = 2 * micro * tok
        ends = jnp.cumsum(rounded(lens))
        meta_own = jnp.concatenate([lens, ends - rounded(lens)])
        x_packed, e_packed = (pack(meta_own, tokens, None, cap) for tokens in (act_in, cot_out))
        ends_other = ends[-1] + jnp.cumsum(rounded(lens_other))
        total = ends_other[-1]
        blocks = (total + BLOCK - 1) // BLOCK
        edge = jnp.stack([total, blocks * BLOCK - total])
        meta_other = jnp.concatenate([lens_other, ends_other - rounded(lens_other), edge])
        x_packed = pack(meta_other, x_other, x_packed, cap)
        e_packed = pack(meta_other, e_other, e_packed, cap)
        meta = jnp.stack([blocks, core]).astype(jnp.int32)

        outs = None
        for j in range(CHUNKS):
            part = chunk_grads(meta, x_packed, e_packed, *weights[j], hidden)
            part = part.reshape(-1, part.shape[-1])
            reduced = lax.psum_scatter(part, 'fsdp', scatter_dimension=0, tiled=True, axis_index_groups=same_core)
            reduced = reduced.reshape(2, hidden, -1)
            away = lax.dynamic_slice_in_dim(reduced[0], (1 - core) * rows_in, rows_in, axis=1)
            got = lax.ppermute(away, 'fsdp', swap)
            outs = place(core_ref, reduced, got, outs, j, chips)
        return outs[0][None], outs[1][None]

    return jax.shard_map(local_step, mesh=mesh, in_specs=(shard_spec, shard_spec, len_spec, weight_spec, weight_spec), out_specs=(shard_spec, shard_spec), check_vma=False)
```

```python
import functools
import math
import jax
import jax.numpy as jnp
from jax import lax
from jax.experimental import pallas as pl
from jax.experimental.pallas import tpu as pltpu
from jax.sharding import PartitionSpec as P


SQRT_HALF = math.sqrt(0.5)
INV_SQRT_TAU = 1.0 / math.sqrt(2.0 * math.pi)

CHUNKS = 4
GATHERS = ((0, 1), (1, 3))
BLOCK = 512
ALIGN = 16
VMEM_LIMIT = 66 * 1024 * 1024 - 2 * 1024 * 1024 - 65536


def pack_kernel(meta, in_ref, *refs, micro, tok, last_call):
    out, buf, sems = refs[-3:]
    k = pl.program_id(0)
    bits = [1 << b for b in range(tok.bit_length() - 1, ALIGN.bit_length() - 2, -1)]

    def segment(step, act):
        slot = lax.rem(step, 2)
        rows = jnp.bitwise_and(meta[step] + (ALIGN - 1), -ALIGN)
        offset = meta[micro + step]
        for bit in bits:
            @pl.when(jnp.bitwise_and(rows, bit) != 0)
            def _():
                first = pl.multiple_of(jnp.bitwise_and(rows, -2 * bit), ALIGN)
                dest = pl.multiple_of(offset + first, ALIGN)
                act(pltpu.make_async_copy(buf.at[slot, pl.ds(first, bit)], out.at[pl.ds(dest, bit)], sems.at[slot]))

    @pl.when(k >= 2)
    def _():
        segment(k - 2, lambda copy: copy.wait())

    slot = lax.rem(k, 2)
    buf[slot] = in_ref[0]
    length = meta[k]
    edge = pl.multiple_of(jnp.minimum(jnp.bitwise_and(length, -ALIGN), tok - ALIGN), ALIGN)
    row = edge + lax.broadcasted_iota(jnp.int32, (ALIGN, buf.shape[-1]), 0)
    kept = jnp.where(row < length, buf[slot, pl.ds(edge, ALIGN)].astype(jnp.float32), 0.0)
    buf[slot, pl.ds(edge, ALIGN)] = kept.astype(buf.dtype)
    segment(k, lambda copy: copy.start())

    @pl.when(k == micro - 1)
    def _():
        segment(k - 1, lambda copy: copy.wait())
        segment(k, lambda copy: copy.wait())
        if last_call:
            total, gap = meta[2 * micro], meta[2 * micro + 1]
            buf[0] = jnp.zeros(buf.shape[1:], buf.dtype)

            def tail(act):
                for bit in bits[1:]:
                    @pl.when(jnp.bitwise_and(gap, bit) != 0)
                    def _():
                        first = jnp.bitwise_and(gap, -2 * bit)
                        dest = pl.multiple_of(total + first, ALIGN)
                        act(pltpu.make_async_copy(buf.at[0, pl.ds(0, bit)], out.at[pl.ds(dest, bit)], sems.at[0]))

            tail(lambda copy: copy.start())
            tail(lambda copy: copy.wait())


def pack(meta, tokens, packed, cap):
    micro, tok, width = tokens.shape
    hbm = pl.BlockSpec(memory_space=pltpu.MemorySpace.HBM)
    given = () if packed is None else (packed,)
    return pl.pallas_call(
        functools.partial(pack_kernel, micro=micro, tok=tok, last_call=packed is not None),
        grid_spec=pltpu.PrefetchScalarGridSpec(
            num_scalar_prefetch=1,
            grid=(micro,),
            in_specs=[pl.BlockSpec((1, tok, width), lambda k, meta: (k, 0, 0))] + [hbm] * len(given),
            out_specs=hbm,
            scratch_shapes=[pltpu.VMEM((2, tok, width), tokens.dtype), pltpu.SemaphoreType.DMA((2,))],
        ),
        out_shape=jax.ShapeDtypeStruct((cap, width), tokens.dtype),
        input_output_aliases={} if packed is None else {2: 0},
        compiler_params=pltpu.CompilerParams(dimension_semantics=("arbitrary",), vmem_limit_bytes=32 * 1024 * 1024),
        cost_estimate=pl.CostEstimate(flops=15_000_000_000, bytes_accessed=4 * tokens.size, transcendentals=0),
        name="pack_own" if packed is None else "pack_partner",
    )(meta, tokens, *given)


def grads_kernel(meta, x_ref, e_ref, *refs, w1_at, w2_at):
    *sources, grads_hbm, w1, w2, acc_i, acc_o, act_t, dpre_t, sems = refs
    i = pl.program_id(0)
    hidden_size, width = w2.shape
    slab_width = sources[0].shape[-1]
    parts = acc_i.shape[0]
    part_width = width // parts
    piece = hidden_size // parts
    block = x_ref.shape[0]

    @pl.when(i == 0)
    def _():
        core, chip = meta[1], meta[2]
        copies = []
        gathered = len(sources) == 2
        for q in range(parts):
            owner = q if gathered else jnp.bitwise_xor(chip, q)
            rows = pl.ds(pl.multiple_of(owner * piece, 8), piece)
            for k in range(2):
                column = pl.multiple_of((2 * owner + (core if k == 0 else 1 - core)) * slab_width, 128)
                if gathered:
                    source = sources[0].at[q, w1_at[0], pl.ds(w1_at[1] + k * hidden_size, hidden_size)]
                else:
                    source = sources[q].at[pl.ds(k * hidden_size, hidden_size)]
                copies.append(pltpu.make_async_copy(source, w1.at[:, pl.ds(column, slab_width)], sems.at[0]))
            if not gathered:
                copies.append(pltpu.make_async_copy(sources[parts + q], w2.at[rows], sems.at[1]))
            elif w2_at is not None:
                for k in range(width // slab_width):
                    source = sources[1].at[q, w2_at[0], pl.ds(w2_at[1] + k * piece, piece)]
                    copies.append(pltpu.make_async_copy(source, w2.at[rows, pl.ds(k * slab_width, slab_width)], sems.at[1]))
        if gathered and w2_at is None:
            copies.append(pltpu.make_async_copy(sources[1], w2, sems.at[1]))
        for copy in copies:
            copy.start()
        acc_i[...] = jnp.zeros_like(acc_i)
        acc_o[...] = jnp.zeros_like(acc_o)
        for copy in copies:
            copy.wait()

    @pl.when(i < meta[0])
    def _():
        sub = 256
        transposed = (((1,), (1,)), ((), ()))

        def hidden(t, carry):
            rows = pl.ds(pl.multiple_of(t * sub, sub), sub)
            pre = lax.dot_general(w1[...], x_ref[rows, :], transposed, preferred_element_type=jnp.float32)
            d_act = lax.dot_general(w2[...], e_ref[rows, :], transposed, preferred_element_type=jnp.float32)
            z = pre.astype(jnp.bfloat16).astype(jnp.float32)
            cdf = 0.5 * (1.0 + lax.erf(z * SQRT_HALF))
            slope = cdf + z * jnp.exp(-0.5 * z * z) * INV_SQRT_TAU
            act_t[:, rows] = (z * cdf).astype(jnp.bfloat16)
            dpre_t[:, rows] = (d_act * slope).astype(jnp.bfloat16)
            return carry

        lax.fori_loop(0, block // sub, hidden, 0)

        def results(p):
            yield pltpu.make_async_copy(acc_i.at[p], grads_hbm.at[p, 0], sems.at[0])
            for q in range(parts):
                yield pltpu.make_async_copy(
                    acc_o.at[p, pl.ds(q * piece, piece)],
                    grads_hbm.at[q, 1, pl.ds(pl.multiple_of(p * piece, 8), piece)], sems.at[1])

        last = i == meta[0] - 1

        def accumulate(p, carry):
            columns = pl.ds(pl.multiple_of(p * part_width, 128), part_width)
            acc_o[p] += jnp.dot(act_t[...], e_ref[:, columns], preferred_element_type=jnp.float32)
            acc_i[p] += jnp.dot(dpre_t[...], x_ref[:, columns], preferred_element_type=jnp.float32)

            @pl.when(last)
            def _():
                for copy in results(p):
                    copy.start()

            return carry

        lax.fori_loop(0, parts, accumulate, 0)

        @pl.when(last)
        def _():
            for p in range(parts):
                for copy in results(p):
                    copy.wait()


def chunk_grads(meta, x_packed, e_packed, sources, w1_at, w2_at, hidden, parts):
    cap, width = x_packed.shape
    hbm = pl.BlockSpec(memory_space=pltpu.MemorySpace.HBM)
    tokens = pl.BlockSpec((BLOCK, width), lambda i, meta: (jnp.minimum(i, meta[0] - 1), 0))
    return pl.pallas_call(
        functools.partial(grads_kernel, w1_at=w1_at, w2_at=w2_at),
        grid_spec=pltpu.PrefetchScalarGridSpec(
            num_scalar_prefetch=1,
            grid=(cap // BLOCK,),
            in_specs=[tokens, tokens] + [hbm] * len(sources),
            out_specs=hbm,
            scratch_shapes=[
                pltpu.VMEM((hidden, width), jnp.bfloat16),
                pltpu.VMEM((hidden, width), jnp.bfloat16),
                pltpu.VMEM((parts, hidden, width // parts), jnp.float32),
                pltpu.VMEM((parts, hidden, width // parts), jnp.float32),
                pltpu.VMEM((hidden, BLOCK), jnp.bfloat16),
                pltpu.VMEM((hidden, BLOCK), jnp.bfloat16),
                pltpu.SemaphoreType.DMA((2,)),
            ],
        ),
        out_shape=jax.ShapeDtypeStruct((parts, 2, hidden, width // parts), jnp.float32),
        compiler_params=pltpu.CompilerParams(dimension_semantics=("arbitrary",), vmem_limit_bytes=VMEM_LIMIT),
        cost_estimate=pl.CostEstimate(flops=8 * 7168 * width * hidden, bytes_accessed=8 * 7168 * width, transcendentals=0),
        name="chunk_grads",
    )(meta, x_packed, e_packed, *sources)


def turn_kernel(core, w_ref, out_ref):
    chunks, piece, _ = out_ref.shape
    for j in range(chunks):
        out_ref[j] = w_ref[:, j * piece:(j + 1) * piece].T


def turned_columns(core, w, other, chips):
    rows, full = w.shape
    per_device = full // (2 * chips)
    piece = per_device // CHUNKS
    return pl.pallas_call(
        turn_kernel,
        grid_spec=pltpu.PrefetchScalarGridSpec(
            num_scalar_prefetch=1,
            grid=(chips,),
            in_specs=[pl.BlockSpec((rows, per_device), lambda q, core: (0, 2 * q + jnp.bitwise_xor(core[0], other)))],
            out_specs=pl.BlockSpec((CHUNKS, piece, rows), lambda q, core: (0, q, 0)),
        ),
        out_shape=jax.ShapeDtypeStruct((CHUNKS, chips * piece, rows), w.dtype),
        compiler_params=pltpu.CompilerParams(dimension_semantics=("arbitrary",)),
        cost_estimate=pl.CostEstimate(flops=3_000_000_000, bytes_accessed=2 * w.size, transcendentals=0),
        name="turn_other" if other else "turn_own",
    )(core, w)


def place_kernel(core, kept_ref, got_ref, rows_ref, *refs):
    gi_ref, go_ref = refs[-2:]
    mine = pl.program_id(1) == core[0]

    @pl.when(mine)
    def _():
        gi_ref[...] = kept_ref[0].T

    @pl.when(jnp.logical_not(mine))
    def _():
        gi_ref[...] = got_ref[...].T

    go_ref[...] = rows_ref[0]


def place(core, reduced, got, outs, j, chips):
    _, hidden, part_width = reduced.shape
    piece = hidden // chips
    rows = part_width // 2
    given = () if outs is None else outs
    anywhere = pl.BlockSpec(memory_space=pltpu.MemorySpace.HBM)
    return pl.pallas_call(
        place_kernel,
        grid_spec=pltpu.PrefetchScalarGridSpec(
            num_scalar_prefetch=1,
            grid=(chips, 2),
            in_specs=[
                pl.BlockSpec((1, piece, rows), lambda q, c, core: (0, q, core[0])),
                pl.BlockSpec((piece, rows), lambda q, c, core: (q, 0)),
                pl.BlockSpec((1, piece, part_width), lambda q, c, core: (1, q, 0)),
            ] + [anywhere] * len(given),
            out_specs=[
                pl.BlockSpec((rows, piece), lambda q, c, core: (0, (2 * q + c) * CHUNKS + j)),
                pl.BlockSpec((piece, part_width), lambda q, c, core: (j, q)),
            ],
        ),
        out_shape=[
            jax.ShapeDtypeStruct((rows, 2 * CHUNKS * hidden), jnp.float32),
            jax.ShapeDtypeStruct((CHUNKS * piece, chips * part_width), jnp.float32),
        ],
        input_output_aliases={} if outs is None else {4: 0, 5: 1},
        compiler_params=pltpu.CompilerParams(dimension_semantics=("arbitrary", "arbitrary")),
        cost_estimate=pl.CostEstimate(flops=2_000_000_000, bytes_accessed=12 * reduced.size, transcendentals=0),
    )(core, reduced, got, reduced, *given)


def solution(mesh):
    shard_spec = P(None, ('rep', 'fsdp'), None)
    len_spec = P(None, ('rep', 'fsdp'))
    weight_spec = P(None, 'fsdp', None)
    count = mesh.shape['fsdp']
    chips = count // 2
    same_core = [[2 * q + c for q in range(chips)] for c in range(2)]
    swap = [(d, d ^ 1) for d in range(count)]

    def local_step(act_in, cot_out, lengths, w_in, w_out):
        micro, tok, width = act_in.shape
        core = lax.rem(lax.axis_index('fsdp'), 2)
        rows_in, rows_out = w_in.shape[1], w_out.shape[1]
        piece = rows_out // CHUNKS
        hidden = chips * piece

        lens = lengths[:, 0]
        lens_other = lax.ppermute(lens, 'fsdp', swap)
        x_sent, e_sent, lens_other = lax.optimization_barrier((act_in, cot_out, lens_other))
        x_other = lax.ppermute(x_sent, 'fsdp', swap)
        e_other = lax.ppermute(e_sent, 'fsdp', swap)

        core_ref = core.reshape(1).astype(jnp.int32)
        w_got = lax.ppermute(turned_columns(core_ref, w_in[0], 1, chips), 'fsdp', swap)
        w_mine = turned_columns(core_ref, w_in[0], 0, chips)

        def gather(slabs):
            shape = slabs.shape
            flat = slabs.reshape(-1, shape[-1])
            flat = lax.all_gather(flat, 'fsdp', axis=0, tiled=True, axis_index_groups=same_core)
            return flat.reshape(chips, *shape)

        w_out_rest = lax.optimization_barrier(w_out)

        def out_rows(first, last):
            rows = w_out_rest[0, first * piece:last * piece].reshape(last - first, piece, width // rows_in, rows_in)
            return rows.transpose(0, 2, 1, 3).reshape(last - first, -1, rows_in)

        weights = []
        for first, last in GATHERS:
            if first == 0:
                w2 = lax.all_gather(w_out[0, :piece], 'fsdp', axis=0, tiled=True, axis_index_groups=same_core)
                w1 = gather(jnp.concatenate([w_mine[:1], w_got[:1]], axis=1))
                weights.append(((w1, w2), (0, 0), None))
            else:
                both = gather(jnp.concatenate([w_mine[first:last], w_got[first:last], out_rows(first, last)], axis=1))
                weights += [((both, both), (n, 0), (n, 2 * hidden)) for n in range(last - first)]

        def rounded(n):
            return (n + (ALIGN - 1)) // ALIGN * ALIGN

        cap = 2 * micro * tok
        ends = jnp.cumsum(rounded(lens))
        meta_own = jnp.concatenate([lens, ends - rounded(lens)])
        x_packed, e_packed = (pack(meta_own, tokens, None, cap) for tokens in (act_in, cot_out))
        ends_other = ends[-1] + jnp.cumsum(rounded(lens_other))
        total = ends_other[-1]
        blocks = (total + BLOCK - 1) // BLOCK
        edge = jnp.stack([total, blocks * BLOCK - total])
        meta_other = jnp.concatenate([lens_other, ends_other - rounded(lens_other), edge])
        x_packed = pack(meta_other, x_other, x_packed, cap)
        e_packed = pack(meta_other, e_other, e_packed, cap)
        across_x = [(d, d ^ 2) for d in range(count)]
        across_y = [(d, d ^ 4) for d in range(count)]
        up = jnp.concatenate([w_mine[-1], w_got[-1]], axis=0)
        down = w_out_rest[0, (CHUNKS - 1) * piece:]
        up, down, e_packed = lax.optimization_barrier((up, down, e_packed))
        up_x, down_y = lax.ppermute(up, 'fsdp', across_x), lax.ppermute(down, 'fsdp', across_y)
        down_x, up_y = lax.ppermute(down, 'fsdp', across_x), lax.ppermute(up, 'fsdp', across_y)
        up_xy, down_xy = lax.ppermute(up_x, 'fsdp', across_y), lax.ppermute(down_y, 'fsdp', across_x)
        weights.append(((up, up_x, up_y, up_xy, down, down_x, down_y, down_xy), None, None))

        meta = jnp.stack([blocks, core, lax.axis_index('fsdp') // 2]).astype(jnp.int32)

        outs = None
        for j in range(CHUNKS):
            part = chunk_grads(meta, x_packed, e_packed, *weights[j], hidden, chips)
            part = part.reshape(-1, part.shape[-1])
            reduced = lax.psum_scatter(part, 'fsdp', scatter_dimension=0, tiled=True, axis_index_groups=same_core)
            reduced = reduced.reshape(2, hidden, -1)
            away = lax.dynamic_slice_in_dim(reduced[0], (1 - core) * rows_in, rows_in, axis=1)
            got = lax.ppermute(away, 'fsdp', swap)
            outs = place(core_ref, reduced, got, outs, j, chips)
        return outs[0][None], outs[1][None]

    return jax.shard_map(local_step, mesh=mesh, in_specs=(shard_spec, shard_spec, len_spec, weight_spec, weight_spec), out_specs=(shard_spec, shard_spec), check_vma=False)
```

```python
import functools
import math
import jax
import jax.numpy as jnp
from jax import lax
from jax.experimental import pallas as pl
from jax.experimental.pallas import tpu as pltpu
from jax.sharding import PartitionSpec as P


SQRT_HALF = math.sqrt(0.5)
INV_SQRT_TAU = 1.0 / math.sqrt(2.0 * math.pi)

CHUNKS = 4
GATHERS = ((0, 1), (1, 2), (2, 4))
BLOCK = 512
ALIGN = 16
VMEM_LIMIT = 66 * 1024 * 1024 - 2 * 1024 * 1024 - 65536


def pack_kernel(meta, in_ref, *refs, micro, tok, last_call):
    out, buf, sems = refs[-3:]
    k = pl.program_id(0)
    bits = [1 << b for b in range(tok.bit_length() - 1, ALIGN.bit_length() - 2, -1)]

    def segment(step, act):
        slot = lax.rem(step, 2)
        rows = jnp.bitwise_and(meta[step] + (ALIGN - 1), -ALIGN)
        offset = meta[micro + step]
        for bit in bits:
            @pl.when(jnp.bitwise_and(rows, bit) != 0)
            def _():
                first = pl.multiple_of(jnp.bitwise_and(rows, -2 * bit), ALIGN)
                dest = pl.multiple_of(offset + first, ALIGN)
                act(pltpu.make_async_copy(buf.at[slot, pl.ds(first, bit)], out.at[pl.ds(dest, bit)], sems.at[slot]))

    @pl.when(k >= 2)
    def _():
        segment(k - 2, lambda copy: copy.wait())

    slot = lax.rem(k, 2)
    buf[slot] = in_ref[0]
    length = meta[k]
    edge = pl.multiple_of(jnp.minimum(jnp.bitwise_and(length, -ALIGN), tok - ALIGN), ALIGN)
    row = edge + lax.broadcasted_iota(jnp.int32, (ALIGN, buf.shape[-1]), 0)
    kept = jnp.where(row < length, buf[slot, pl.ds(edge, ALIGN)].astype(jnp.float32), 0.0)
    buf[slot, pl.ds(edge, ALIGN)] = kept.astype(buf.dtype)
    segment(k, lambda copy: copy.start())

    @pl.when(k == micro - 1)
    def _():
        segment(k - 1, lambda copy: copy.wait())
        segment(k, lambda copy: copy.wait())
        if last_call:
            total, gap = meta[2 * micro], meta[2 * micro + 1]
            buf[0] = jnp.zeros(buf.shape[1:], buf.dtype)

            def tail(act):
                for bit in bits[1:]:
                    @pl.when(jnp.bitwise_and(gap, bit) != 0)
                    def _():
                        first = jnp.bitwise_and(gap, -2 * bit)
                        dest = pl.multiple_of(total + first, ALIGN)
                        act(pltpu.make_async_copy(buf.at[0, pl.ds(0, bit)], out.at[pl.ds(dest, bit)], sems.at[0]))

            tail(lambda copy: copy.start())
            tail(lambda copy: copy.wait())


def pack(meta, tokens, packed, cap):
    micro, tok, width = tokens.shape
    hbm = pl.BlockSpec(memory_space=pltpu.MemorySpace.HBM)
    given = () if packed is None else (packed,)
    return pl.pallas_call(
        functools.partial(pack_kernel, micro=micro, tok=tok, last_call=packed is not None),
        grid_spec=pltpu.PrefetchScalarGridSpec(
            num_scalar_prefetch=1,
            grid=(micro,),
            in_specs=[pl.BlockSpec((1, tok, width), lambda k, meta: (k, 0, 0))] + [hbm] * len(given),
            out_specs=hbm,
            scratch_shapes=[pltpu.VMEM((2, tok, width), tokens.dtype), pltpu.SemaphoreType.DMA((2,))],
        ),
        out_shape=jax.ShapeDtypeStruct((cap, width), tokens.dtype),
        input_output_aliases={} if packed is None else {2: 0},
        compiler_params=pltpu.CompilerParams(dimension_semantics=("arbitrary",), vmem_limit_bytes=32 * 1024 * 1024),
        cost_estimate=pl.CostEstimate(flops=15_000_000_000, bytes_accessed=4 * tokens.size, transcendentals=0),
        name="pack_own" if packed is None else "pack_partner",
    )(meta, tokens, *given)


def grads_kernel(meta, x_ref, e_ref, w1_hbm, w2_hbm, *refs, w1_at, w2_at):
    *outs, w1, w2, acc_i, acc_o, act_t, dpre_t, sems = refs
    grads_hbm = outs[0]
    i = pl.program_id(0)
    hidden_size, width = w2.shape
    slab_width = w1_hbm.shape[-1]
    parts = acc_i.shape[0]
    part_width = width // parts
    piece = hidden_size // parts
    block = x_ref.shape[0]

    @pl.when(i == 0)
    def _():
        core = meta[1]
        copies = []
        for q in range(parts):
            for k in range(2):
                column = pl.multiple_of((2 * q + (core if k == 0 else 1 - core)) * slab_width, 128)
                source = w1_hbm.at[q, w1_at[0], pl.ds(w1_at[1] + k * hidden_size, hidden_size)]
                copies.append(pltpu.make_async_copy(source, w1.at[:, pl.ds(column, slab_width)], sems.at[0]))
            if w2_at is None:
                continue
            for k in range(width // slab_width):
                source = w2_hbm.at[q, w2_at[0], pl.ds(w2_at[1] + k * piece, piece)]
                copies.append(pltpu.make_async_copy(source, w2.at[pl.ds(q * piece, piece), pl.ds(k * slab_width, slab_width)], sems.at[1]))
        if w2_at is None:
            copies.append(pltpu.make_async_copy(w2_hbm, w2, sems.at[1]))
        for copy in copies:
            copy.start()
        acc_i[...] = jnp.zeros_like(acc_i)
        acc_o[...] = jnp.zeros_like(acc_o)
        for copy in copies:
            copy.wait()

    @pl.when(i < meta[0])
    def _():
        sub = 256
        transposed = (((1,), (1,)), ((), ()))

        def hidden(t, carry):
            rows = pl.ds(pl.multiple_of(t * sub, sub), sub)
            pre = lax.dot_general(w1[...], x_ref[rows, :], transposed, preferred_element_type=jnp.float32)
            d_act = lax.dot_general(w2[...], e_ref[rows, :], transposed, preferred_element_type=jnp.float32)
            z = pre.astype(jnp.bfloat16).astype(jnp.float32)
            cdf = 0.5 * (1.0 + lax.erf(z * SQRT_HALF))
            slope = cdf + z * jnp.exp(-0.5 * z * z) * INV_SQRT_TAU
            act_t[:, rows] = (z * cdf).astype(jnp.bfloat16)
            dpre_t[:, rows] = (d_act * slope).astype(jnp.bfloat16)
            return carry

        lax.fori_loop(0, block // sub, hidden, 0)

        def results(p):
            if len(outs) == 2:
                half = part_width // 2
                for rows, dest in ((meta[1], grads_hbm.at[p, pl.ds(0, hidden_size)]), (1 - meta[1], outs[1].at[p])):
                    columns = pl.ds(pl.multiple_of(rows * half, 128), half)
                    yield pltpu.make_async_copy(acc_i.at[p, :, columns], dest, sems.at[0])
                for q in range(parts):
                    for h in range(2):
                        first = pl.multiple_of(2 * hidden_size + (2 * p + h) * piece, 8)
                        yield pltpu.make_async_copy(
                            acc_o.at[p, pl.ds(q * piece, piece), pl.ds(h * half, half)],
                            grads_hbm.at[q, pl.ds(first, piece)], sems.at[1])
                return
            yield pltpu.make_async_copy(acc_i.at[p], grads_hbm.at[p, 0], sems.at[0])
            for q in range(parts):
                yield pltpu.make_async_copy(
                    acc_o.at[p, pl.ds(q * piece, piece)],
                    grads_hbm.at[q, 1, pl.ds(pl.multiple_of(p * piece, 8), piece)], sems.at[1])

        last = i == meta[0] - 1

        def accumulate(p, carry):
            columns = pl.ds(pl.multiple_of(p * part_width, 128), part_width)
            acc_o[p] += jnp.dot(act_t[...], e_ref[:, columns], preferred_element_type=jnp.float32)
            acc_i[p] += jnp.dot(dpre_t[...], x_ref[:, columns], preferred_element_type=jnp.float32)

            @pl.when(last)
            def _():
                for copy in results(p):
                    copy.start()

            return carry

        lax.fori_loop(0, parts, accumulate, 0)

        @pl.when(last)
        def _():
            for p in range(parts):
                for copy in results(p):
                    copy.wait()


def chunk_grads(meta, x_packed, e_packed, w1_from, w1_at, w2_from, w2_at, hidden, halves):
    cap, width = x_packed.shape
    parts = w1_from.shape[0]
    hbm = pl.BlockSpec(memory_space=pltpu.MemorySpace.HBM)
    tokens = pl.BlockSpec((BLOCK, width), lambda i, meta: (jnp.minimum(i, meta[0] - 1), 0))
    part_width = width // parts
    if halves:
        shapes = [(parts, 4 * hidden, part_width // 2), (parts, hidden, part_width // 2)]
    else:
        shapes = [(parts, 2, hidden, part_width)]
    return pl.pallas_call(
        functools.partial(grads_kernel, w1_at=w1_at, w2_at=w2_at),
        grid_spec=pltpu.PrefetchScalarGridSpec(
            num_scalar_prefetch=1,
            grid=(cap // BLOCK,),
            in_specs=[tokens, tokens, hbm, hbm],
            out_specs=[hbm] * len(shapes),
            scratch_shapes=[
                pltpu.VMEM((hidden, width), jnp.bfloat16),
                pltpu.VMEM((hidden, width), jnp.bfloat16),
                pltpu.VMEM((parts, hidden, width // parts), jnp.float32),
                pltpu.VMEM((parts, hidden, width // parts), jnp.float32),
                pltpu.VMEM((hidden, BLOCK), jnp.bfloat16),
                pltpu.VMEM((hidden, BLOCK), jnp.bfloat16),
                pltpu.SemaphoreType.DMA((2,)),
            ],
        ),
        out_shape=[jax.ShapeDtypeStruct(shape, jnp.float32) for shape in shapes],
        compiler_params=pltpu.CompilerParams(dimension_semantics=("arbitrary",), vmem_limit_bytes=VMEM_LIMIT),
        cost_estimate=pl.CostEstimate(flops=8 * 7168 * width * hidden, bytes_accessed=8 * 7168 * width, transcendentals=0),
        name="chunk_grads",
    )(meta, x_packed, e_packed, w1_from, w2_from)


def turn_kernel(core, w_ref, out_ref):
    chunks, piece, _ = out_ref.shape
    for j in range(chunks):
        out_ref[j] = w_ref[:, j * piece:(j + 1) * piece].T


def turned_columns(core, w, other, chips):
    rows, full = w.shape
    per_device = full // (2 * chips)
    piece = per_device // CHUNKS
    return pl.pallas_call(
        turn_kernel,
        grid_spec=pltpu.PrefetchScalarGridSpec(
            num_scalar_prefetch=1,
            grid=(chips,),
            in_specs=[pl.BlockSpec((rows, per_device), lambda q, core: (0, 2 * q + jnp.bitwise_xor(core[0], other)))],
            out_specs=pl.BlockSpec((CHUNKS, piece, rows), lambda q, core: (0, q, 0)),
        ),
        out_shape=jax.ShapeDtypeStruct((CHUNKS, chips * piece, rows), w.dtype),
        compiler_params=pltpu.CompilerParams(dimension_semantics=("arbitrary",)),
        cost_estimate=pl.CostEstimate(flops=3_000_000_000, bytes_accessed=2 * w.size, transcendentals=0),
        name="turn_other" if other else "turn_own",
    )(core, w)


def place_kernel(core, kept_ref, got_ref, rows_ref, *refs):
    gi_ref, go_ref = refs[-2:]
    mine = pl.program_id(1) == core[0]

    @pl.when(mine)
    def _():
        gi_ref[...] = kept_ref[0].T

    @pl.when(jnp.logical_not(mine))
    def _():
        gi_ref[...] = got_ref[...].T

    go_ref[...] = rows_ref[0]


def place(core, reduced, got, outs, j, chips):
    _, hidden, part_width = reduced.shape
    piece = hidden // chips
    rows = part_width // 2
    given = () if outs is None else outs
    anywhere = pl.BlockSpec(memory_space=pltpu.MemorySpace.HBM)
    return pl.pallas_call(
        place_kernel,
        grid_spec=pltpu.PrefetchScalarGridSpec(
            num_scalar_prefetch=1,
            grid=(chips, 2),
            in_specs=[
                pl.BlockSpec((1, piece, rows), lambda q, c, core: (0, q, core[0])),
                pl.BlockSpec((piece, rows), lambda q, c, core: (q, 0)),
                pl.BlockSpec((1, piece, part_width), lambda q, c, core: (1, q, 0)),
            ] + [anywhere] * len(given),
            out_specs=[
                pl.BlockSpec((rows, piece), lambda q, c, core: (0, (2 * q + c) * CHUNKS + j)),
                pl.BlockSpec((piece, part_width), lambda q, c, core: (j, q)),
            ],
        ),
        out_shape=[
            jax.ShapeDtypeStruct((rows, 2 * CHUNKS * hidden), jnp.float32),
            jax.ShapeDtypeStruct((CHUNKS * piece, chips * part_width), jnp.float32),
        ],
        input_output_aliases={} if outs is None else {4: 0, 5: 1},
        compiler_params=pltpu.CompilerParams(dimension_semantics=("arbitrary", "arbitrary")),
        cost_estimate=pl.CostEstimate(flops=2_000_000_000, bytes_accessed=12 * reduced.size, transcendentals=0),
    )(core, reduced, got, reduced, *given)


def place_last_kernel(core, reduced, gi_in, go_in, gi, go, buf, turned, in_sems, out_sems, *, j):
    del gi_in, go_in
    blocks, piece, half = buf.shape
    chips = blocks // 4
    loads = [pltpu.make_async_copy(reduced.at[pl.ds(b * piece, piece)], buf.at[b], in_sems.at[b]) for b in range(blocks)]
    for load in loads:
        load.start()
    stores = []
    for b in range(2 * chips):
        side = core[0] if b < chips else 1 - core[0]
        column = pl.multiple_of(((2 * (b % chips) + side) * CHUNKS + j) * piece, 128)
        loads[b].wait()
        turned[b] = buf[b].T
        stores.append(pltpu.make_async_copy(turned.at[b], gi.at[:, pl.ds(column, piece)], out_sems.at[b]))
        stores[-1].start()
    for b in range(2 * chips, blocks):
        loads[b].wait()
        dest = go.at[pl.ds(j * piece, piece), pl.ds((b - 2 * chips) * half, half)]
        stores.append(pltpu.make_async_copy(buf.at[b], dest, out_sems.at[b]))
        stores[-1].start()
    for store in stores:
        store.wait()


def place_last(core, reduced, outs, j, chips):
    rows, half = reduced.shape
    blocks = 4 * chips
    piece = rows // blocks
    anywhere = pl.BlockSpec(memory_space=pltpu.MemorySpace.HBM)
    return pl.pallas_call(
        functools.partial(place_last_kernel, j=j),
        grid_spec=pltpu.PrefetchScalarGridSpec(
            num_scalar_prefetch=1,
            grid=(),
            in_specs=[anywhere] * 3,
            out_specs=[anywhere] * 2,
            scratch_shapes=[
                pltpu.VMEM((blocks, piece, half), jnp.float32),
                pltpu.VMEM((2 * chips, half, piece), jnp.float32),
                pltpu.SemaphoreType.DMA((blocks,)),
                pltpu.SemaphoreType.DMA((blocks,)),
            ],
        ),
        out_shape=[jax.ShapeDtypeStruct(out.shape, out.dtype) for out in outs],
        input_output_aliases={2: 0, 3: 1},
        compiler_params=pltpu.CompilerParams(vmem_limit_bytes=VMEM_LIMIT),
        cost_estimate=pl.CostEstimate(flops=2_000_000_000, bytes_accessed=8 * reduced.size, transcendentals=0),
    )(core, reduced, *outs)


def solution(mesh):
    shard_spec = P(None, ('rep', 'fsdp'), None)
    len_spec = P(None, ('rep', 'fsdp'))
    weight_spec = P(None, 'fsdp', None)
    count = mesh.shape['fsdp']
    chips = count // 2
    same_core = [[2 * q + c for q in range(chips)] for c in range(2)]
    swap = [(d, d ^ 1) for d in range(count)]

    def local_step(act_in, cot_out, lengths, w_in, w_out):
        micro, tok, width = act_in.shape
        core = lax.rem(lax.axis_index('fsdp'), 2)
        rows_in, rows_out = w_in.shape[1], w_out.shape[1]
        piece = rows_out // CHUNKS
        hidden = chips * piece

        lens = lengths[:, 0]
        lens_other = lax.ppermute(lens, 'fsdp', swap)
        x_sent, e_sent, lens_other = lax.optimization_barrier((act_in, cot_out, lens_other))
        x_other = lax.ppermute(x_sent, 'fsdp', swap)
        e_other = lax.ppermute(e_sent, 'fsdp', swap)

        core_ref = core.reshape(1).astype(jnp.int32)
        w_got = lax.ppermute(turned_columns(core_ref, w_in[0], 1, chips), 'fsdp', swap)
        w_mine = turned_columns(core_ref, w_in[0], 0, chips)

        def gather(slabs):
            shape = slabs.shape
            flat = slabs.reshape(-1, shape[-1])
            flat = lax.all_gather(flat, 'fsdp', axis=0, tiled=True, axis_index_groups=same_core)
            return flat.reshape(chips, *shape)

        def out_rows(first, last):
            rows = w_out[0, first * piece:last * piece].reshape(last - first, piece, width // rows_in, rows_in)
            return rows.transpose(0, 2, 1, 3).reshape(last - first, -1, rows_in)

        weights = []
        for first, last in GATHERS:
            if first == 0:
                w2 = lax.all_gather(w_out[0, :piece], 'fsdp', axis=0, tiled=True, axis_index_groups=same_core)
                w1 = gather(jnp.concatenate([w_mine[:1], w_got[:1]], axis=1))
                weights.append((w1, (0, 0), w2, None))
            else:
                both = gather(jnp.concatenate([w_mine[first:last], w_got[first:last], out_rows(first, last)], axis=1))
                weights += [(both, (n, 0), both, (n, 2 * hidden)) for n in range(last - first)]

        def rounded(n):
            return (n + (ALIGN - 1)) // ALIGN * ALIGN

        cap = 2 * micro * tok
        ends = jnp.cumsum(rounded(lens))
        meta_own = jnp.concatenate([lens, ends - rounded(lens)])
        x_packed, e_packed = (pack(meta_own, tokens, None, cap) for tokens in (act_in, cot_out))
        ends_other = ends[-1] + jnp.cumsum(rounded(lens_other))
        total = ends_other[-1]
        blocks = (total + BLOCK - 1) // BLOCK
        edge = jnp.stack([total, blocks * BLOCK - total])
        meta_other = jnp.concatenate([lens_other, ends_other - rounded(lens_other), edge])
        x_packed = pack(meta_other, x_other, x_packed, cap)
        e_packed = pack(meta_other, e_other, e_packed, cap)
        meta = jnp.stack([blocks, core]).astype(jnp.int32)

        outs = None
        for j in range(CHUNKS):
            halves = j == CHUNKS - 1
            part, *away = chunk_grads(meta, x_packed, e_packed, *weights[j], hidden, halves)
            if halves:
                part = lax.dynamic_update_slice_in_dim(part, lax.ppermute(away[0], 'fsdp', swap), hidden, axis=1)
            part = part.reshape(-1, part.shape[-1])
            reduced = lax.psum_scatter(part, 'fsdp', scatter_dimension=0, tiled=True, axis_index_groups=same_core)
            if halves:
                outs = place_last(core_ref, reduced, outs, j, chips)
                break
            reduced = reduced.reshape(2, hidden, -1)
            away = lax.dynamic_slice_in_dim(reduced[0], (1 - core) * rows_in, rows_in, axis=1)
            got = lax.ppermute(away, 'fsdp', swap)
            outs = place(core_ref, reduced, got, outs, j, chips)
        return outs[0][None], outs[1][None]

    return jax.shard_map(local_step, mesh=mesh, in_specs=(shard_spec, shard_spec, len_spec, weight_spec, weight_spec), out_specs=(shard_spec, shard_spec), check_vma=False)
```
